16 devices in a mesh: dp: 4 (over y, z, core), tp: 4 (over x).
Axes of the slice: x: 4, y: 2, z: 1, core: 2. Of those that a mesh axis runs over, the one named last changes fastest.
The devices are a block of a 4x4x8 slice.
Arguments:
- x: bfloat16 [4, 2048, 2048], P('dp', 'tp'), parts along dimension 0
- dy: bfloat16 [4, 2048, 2048], P('dp', 'tp'), parts along dimension 0
- wq: bfloat16 [2048, 2048], P(None, 'tp')
- wk: bfloat16 [2048, 2048], P(None, 'tp')
- wv: bfloat16 [2048, 2048], P(None, 'tp')
- wo: bfloat16 [2048, 2048], P('tp')
- w_gate: bfloat16 [2048, 8192], P(None, 'tp')
- w_up: bfloat16 [2048, 8192], P(None, 'tp')
- w_down: bfloat16 [8192, 2048], P('tp')
Outputs:
- output 1: bfloat16 [4, 2048, 2048], P('dp', 'tp'), parts along dimension 0
- output 2: bfloat16 [8192, 2048], P('dp', 'tp'), parts along dimension 0
- output 3: bfloat16 [8192, 2048], P('dp', 'tp'), parts along dimension 0
- output 4: bfloat16 [8192, 2048], P('dp', 'tp'), parts along dimension 0
- output 5: bfloat16 [8192, 2048], P(('dp', 'tp')), parts along dimension 0
- output 6: bfloat16 [8192, 8192], P('dp', 'tp'), parts along dimension 0
- output 7: bfloat16 [8192, 8192], P('dp', 'tp'), parts along dimension 0
- output 8: bfloat16 [32768, 2048], P(('dp', 'tp')), parts along dimension 0
There are 4 independent parts. The reference program is written for one: setup_inputs(seed, part) draws one part's arguments, and reference() takes and returns one part's arrays. A program takes and returns all parts, laid end to end along the dimension named above; an argument that names none is the same for every part.
All inputs are finite; a program needn't handle non-finite values.
Results may differ from the reference program's by a relative error of at most 0.024.
Values are sent between devices in bfloat16 or wider.
A program may use at most 768 MiB of HBM per device.

```python
import jax
import jax.numpy as jnp
from jax import lax

SEQUENCES = 1
TOKENS = 2048
D = 2048
HEADS = 16
KV_HEADS = 16
HEAD = 128
FF = 8192
THETA = 10000
NAMES = ("wq", "wk", "wv", "wo", "w_gate", "w_up", "w_down")
SHAPES = {
    "wq": (D, HEADS * HEAD),
    "wk": (D, KV_HEADS * HEAD),
    "wv": (D, KV_HEADS * HEAD),
    "wo": (HEADS * HEAD, D),
    "w_gate": (D, FF),
    "w_up": (D, FF),
    "w_down": (FF, D),
}


def bump(key, n, height):
    away = (jnp.arange(n, dtype=jnp.int32) - jax.random.randint(key, (), 0, n, jnp.int32)) % n
    return jnp.where(away < n // 8, height, 1.0)


def together(key, own, strength):
    shared = jax.random.normal(key, own.shape[1:], jnp.float32)
    return (own + strength * shared) * lax.rsqrt(1 + strength * strength)


def setup_inputs(seed: int = 0, part: int = 0) -> dict:
    kx, kdy, ka, kb, kz, kf, kh, kl, *kw = jax.random.split(jax.random.key(seed), 8 + len(NAMES))
    kx, kdy, ka, kb = (jax.random.fold_in(k, part) for k in (kx, kdy, ka, kb))
    shape = (SEQUENCES, TOKENS, D)
    much_x, much_dy = jax.random.uniform(kz, (2,), jnp.float32, 0.0, 1.0)
    loud = 2.0 ** jax.random.uniform(jax.random.fold_in(kz, 1), (), jnp.float32, -1.0, 2.0)
    halves = 2.0 ** jax.random.uniform(kl, (2,), jnp.float32, -1.0, 1.0)
    times = {"wq": 1.0, "wk": 1.0, "wv": 2.0, "wo": halves[0], "w_gate": 1.0, "w_up": bump(kh, FF, 4.0), "w_down": halves[1]}
    x = together(ka, jax.random.normal(kx, shape, jnp.float32), much_x) * bump(kf, D, 4.0)
    dy = together(kb, jax.random.normal(kdy, shape, jnp.float32), much_dy)
    drawn = {"x": x.astype(jnp.bfloat16), "dy": (loud * dy * (SEQUENCES * TOKENS) ** -0.5).astype(jnp.bfloat16)}
    for key, name in zip(kw, NAMES, strict=True):
        drawn[name] = (jax.random.normal(key, SHAPES[name], jnp.float32) * SHAPES[name][0] ** -0.5 * times[name]).astype(jnp.bfloat16)
    return drawn


def matmul(a, w):
    return jnp.dot(a, w, preferred_element_type=jnp.float32).astype(jnp.bfloat16)


def normed(h):
    wide = h.astype(jnp.float32)
    scale = lax.rsqrt(jnp.mean(wide**2, -1, keepdims=True) + 1e-6)
    return (wide * scale).astype(jnp.bfloat16)


def turned(t, theta):
    half = t.shape[-1] // 2
    angle = jnp.arange(t.shape[0], dtype=jnp.float32)[:, None] * theta ** (-jnp.arange(half, dtype=jnp.float32) / half)
    cos, sin = jnp.cos(angle)[:, None], jnp.sin(angle)[:, None]
    a, b = t[..., :half].astype(jnp.float32), t[..., half:].astype(jnp.float32)
    return jnp.concatenate([a * cos - b * sin, b * cos + a * sin], -1).astype(jnp.bfloat16)


def seen_by(q, k, v):
    tokens, kv = q.shape[0], k.shape[1]
    q = q.reshape(tokens, kv, -1, q.shape[-1])
    scores = jnp.einsum("tgsd,ugd->gstu", q.astype(jnp.float32), k.astype(jnp.float32)) * q.shape[-1] ** -0.5
    place = jnp.arange(tokens)
    weights = jax.nn.softmax(jnp.where(place[:, None] >= place, scores, -jnp.inf), -1).astype(jnp.bfloat16)
    return jnp.einsum("gstu,ugd->tgsd", weights.astype(jnp.float32), v.astype(jnp.float32)).astype(jnp.bfloat16).reshape(tokens, -1)


def layer(h, w):
    a = normed(h)
    q, k = (turned(matmul(a, w[name]).reshape(h.shape[0], -1, HEAD), THETA) for name in ("wq", "wk"))
    h = h + matmul(seen_by(q, k, matmul(a, w["wv"]).reshape(h.shape[0], -1, HEAD)), w["wo"])
    b = normed(h)
    gate = jnp.dot(b, w["w_gate"], preferred_element_type=jnp.float32)
    up = jnp.dot(b, w["w_up"], preferred_element_type=jnp.float32)
    return h + matmul((jax.nn.silu(gate) * up).astype(jnp.bfloat16), w["w_down"])


def reference(x, dy, wq, wk, wv, wo, w_gate, w_up, w_down):
    weights = dict(zip(NAMES, (wq, wk, wv, wo, w_gate, w_up, w_down), strict=True))

    def take(so_far, sequence):
        h, by_y = sequence
        _, back = jax.vjp(lambda w, h: layer(h, w), weights, h)
        by_weights, by_h = back(by_y)
        return jax.tree.map(lambda total, term: total + term.astype(jnp.float32), so_far, by_weights), by_h

    none_yet = {name: jnp.zeros(w.shape, jnp.float32) for name, w in weights.items()}
    by_weights, by_x = lax.scan(take, none_yet, (x, dy))
    return (by_x, *(by_weights[name].astype(jnp.bfloat16) for name in NAMES))
```

```python
import functools

import jax
import jax.numpy as jnp
from jax import lax
from jax.experimental import pallas as pl
from jax.experimental.pallas import tpu as pltpu
from jax.sharding import PartitionSpec as P

NEG = -1e30
HIDDEN = 2 * NEG
LOG2E = 1.4426950408889634
VMEM = 60 * 2**20
HEAD = 128
THETA = 10000
NAMES = ("wq", "wk", "wv", "wo", "w_gate", "w_up", "w_down")


def _dot(a, b, ca, cb):
    return lax.dot_general(a, b, (((ca,), (cb,)), ((), ())), preferred_element_type=jnp.float32)


def _gap(bk, bq):
    return lax.broadcasted_iota(jnp.int32, (bk, bq), 1) - lax.broadcasted_iota(jnp.int32, (bk, bq), 0)


def _turn(t, cos, sin):
    return t * cos + pltpu.roll(t, HEAD // 2, 1) * sin


def _head(i):
    return slice(i * HEAD, (i + 1) * HEAD)


def _attend(q_ref, k_ref, v_ref, cos_ref, sin_ref, o_ref, lse_ref, qr_ref, kr_ref, top_s, mix_s, gap_s, *, scale, bk, strip):
    heads, bq = o_ref.shape[1] // HEAD, o_ref.shape[0]
    iq = pl.program_id(0)
    e = scale * LOG2E
    low = q_ref.dtype
    mine = pl.ds(pl.multiple_of(iq * bq, bq), bq)

    @pl.when(iq == 0)
    def _():
        gap_s[...] = _gap(bk, strip)

    cos, sin = cos_ref[...], sin_ref[...]
    for i in range(heads):
        qr_ref[:, _head(i)] = _turn(q_ref[:, _head(i)].astype(jnp.float32), cos, sin).astype(low)
        kr_ref[mine, _head(i)] = _turn(k_ref[:, _head(i)].astype(jnp.float32), cos, sin).astype(low)
    top_s[...] = jnp.full_like(top_s, NEG)
    mix_s[...] = jnp.zeros_like(mix_s)
    ones = jnp.ones((8, bk), low)
    pieces = [(i, at) for i in range(heads) for at in range(0, bq, strip)]

    def block(j, pieces, edge):
        here = pl.ds(pl.multiple_of(j * bk, bk), bk)
        scores = [_dot(kr_ref[here, _head(i)], qr_ref[at : at + strip, _head(i)], 1, 1) for i, at in pieces]
        weights, keeps = [], []
        for (i, at), s in zip(pieces, scores):
            if at == edge:
                s = jnp.where(gap_s[...] >= 0, s, HIDDEN)
            old = top_s[i : i + 1, at : at + strip]
            top = jnp.maximum(old, s.max(axis=0, keepdims=True))
            top_s[i : i + 1, at : at + strip] = top
            weights.append(jnp.exp2((s - top) * e).astype(low))
            keeps.append(jnp.exp2((old - top) * e))
        for (i, at), p, keep in zip(pieces, weights, keeps):
            values = jnp.concatenate([v_ref[here, _head(i)].T, ones], axis=0)
            mix_s[i, :, at : at + strip] = mix_s[i, :, at : at + strip] * keep + _dot(values, p, 1, 0)

    first = iq * (bq // bk)
    lax.fori_loop(0, first, lambda j, _: block(j, pieces, None), None)
    for n in range(bq // bk):
        block(first + n, [(i, at) for i, at in pieces if at >= n * bk], n * bk)
    for i in range(heads):
        top, total = top_s[i : i + 1, :], mix_s[i, HEAD : HEAD + 1, :]
        o_ref[:, _head(i)] = (mix_s[i, :HEAD, :] * (1 / total)).T.astype(o_ref.dtype)
        lse_ref[i : i + 1, :] = top * scale + jnp.log(total)


def attend(qkv, cos, sin, bq=1024, bk=512, strip=512):
    tokens, width = qkv.shape[0], qkv.shape[1] // 3
    heads = width // HEAD
    rows = lambda c: pl.BlockSpec((bq, width), lambda i: (i, c))
    angle = pl.BlockSpec((bq, HEAD), lambda i: (i, 0))
    flat = jax.ShapeDtypeStruct((tokens, width), qkv.dtype)
    return pl.pallas_call(
        functools.partial(_attend, scale=HEAD**-0.5, bk=bk, strip=strip),
        grid=(tokens // bq,),
        in_specs=[rows(0), rows(1), pl.BlockSpec((tokens, width), lambda i: (0, 2)), angle, angle],
        out_specs=[rows(0), pl.BlockSpec((heads, bq), lambda i: (0, i)), rows(0), pl.BlockSpec((tokens, width), lambda i: (0, 0))],
        out_shape=[flat, jax.ShapeDtypeStruct((heads, tokens), jnp.float32), flat, flat],
        scratch_shapes=[pltpu.VMEM((heads, bq), jnp.float32), pltpu.VMEM((heads, HEAD + 8, bq), jnp.float32), pltpu.VMEM((bk, strip), jnp.int32)],
        compiler_params=pltpu.CompilerParams(dimension_semantics=("arbitrary",), vmem_limit_bytes=VMEM),
        cost_estimate=pl.CostEstimate(flops=4 * tokens * tokens * width, transcendentals=heads * tokens * tokens, bytes_accessed=16 * tokens * width),
    )(qkv, qkv, qkv, cos, sin)


def _attend_back(q_ref, k_ref, v_ref, do_ref, o_ref, lse_ref, cos_ref, sin_ref, d_ref, dq_s, dk_s, dv_s, gap_s, *, scale, bk, edge):
    heads, bq = q_ref.shape[1] // HEAD, q_ref.shape[0]
    iq = pl.program_id(0)
    e = scale * LOG2E
    low = q_ref.dtype
    mine = pl.ds(pl.multiple_of(iq * bq, bq), bq)

    @pl.when(iq == 0)
    def _():
        gap_s[...] = _gap(edge, bq)
        dk_s[...] = jnp.zeros_like(dk_s)
        dv_s[...] = jnp.zeros_like(dv_s)

    dq_s[...] = jnp.zeros_like(dq_s)
    lses = [lse_ref[i : i + 1, :] * LOG2E for i in range(heads)]
    deltas = [
        (do_ref[:, _head(i)].astype(jnp.float32) * o_ref[:, _head(i)].astype(jnp.float32)).T.sum(axis=0, keepdims=True) for i in range(heads)
    ]

    def block(start, keys, skip, masked):
        here = pl.ds(pl.multiple_of(start, keys), keys)
        qs = [q_ref[skip:, _head(i)] for i in range(heads)]
        dos = [do_ref[skip:, _head(i)] for i in range(heads)]
        scores = [_dot(k_ref[here, _head(i)], qs[i], 1, 1) for i in range(heads)]
        dps = [_dot(v_ref[here, _head(i)], dos[i], 1, 1) for i in range(heads)]
        for i in range(heads):
            p = jnp.exp2(scores[i] * e - lses[i][:, skip:])
            if masked:
                p = jnp.where(gap_s[:keys, : bq - skip] >= 0, p, 0.0)
            ds = (p * (dps[i] - deltas[i][:, skip:])).astype(low)
            dv_s[i, here, :] += _dot(p.astype(low), dos[i], 1, 0)
            dk_s[i, here, :] += _dot(ds, qs[i], 1, 0)
            dq_s[i, :, skip:] += _dot(k_ref[here, _head(i)].T, ds, 1, 0)

    lax.fori_loop(0, iq * (bq // bk), lambda j, _: block(j * bk, bk, 0, False), None)
    for skip in range(0, bq, edge):
        block(iq * bq + skip, edge, skip, True)
    cos, sin = cos_ref[mine, :], sin_ref[mine, :]
    for i in range(heads):
        d_ref[mine, _head(i)] = _turn((dq_s[i] * scale).T, cos, -sin).astype(low)

    @pl.when(iq == pl.num_programs(0) - 1)
    def _():
        for i in range(heads):
            d_ref[:, _head(heads + i)] = _turn(dk_s[i] * scale, cos_ref[...], -sin_ref[...]).astype(low)
            d_ref[:, _head(2 * heads + i)] = dv_s[i].astype(low)


def attend_back(q, k, qkv, d_out, out, lse, cos, sin, bq=512, bk=512, edge=256):
    tokens, width = q.shape
    heads = width // HEAD
    rows = pl.BlockSpec((bq, width), lambda i: (i, 0))
    every = lambda c: pl.BlockSpec((tokens, width), lambda i: (0, c))
    angle = pl.BlockSpec((tokens, HEAD), lambda i: (0, 0))
    return pl.pallas_call(
        functools.partial(_attend_back, scale=HEAD**-0.5, bk=bk, edge=edge),
        grid=(tokens // bq,),
        in_specs=[rows, every(0), every(2), rows, rows, pl.BlockSpec((heads, bq), lambda i: (0, i)), angle, angle],
        out_specs=pl.BlockSpec((tokens, 3 * width), lambda i: (0, 0)),
        out_shape=jax.ShapeDtypeStruct((tokens, 3 * width), q.dtype),
        scratch_shapes=[pltpu.VMEM((heads, HEAD, bq), jnp.float32), pltpu.VMEM((heads, tokens, HEAD), jnp.float32),
                        pltpu.VMEM((heads, tokens, HEAD), jnp.float32), pltpu.VMEM((edge, bq), jnp.int32)],
        compiler_params=pltpu.CompilerParams(dimension_semantics=("arbitrary",), vmem_limit_bytes=VMEM),
        cost_estimate=pl.CostEstimate(flops=10 * tokens * tokens * width, transcendentals=heads * tokens * tokens, bytes_accessed=18 * tokens * width),
    )(q, k, qkv, d_out, out, lse, cos, sin)


def angles(tokens):
    half = HEAD // 2
    angle = jnp.arange(tokens, dtype=jnp.float32)[:, None] * THETA ** (-jnp.arange(half, dtype=jnp.float32) / half)
    cos, sin = jnp.cos(angle), jnp.sin(angle)
    return jnp.concatenate([cos, cos], 1), jnp.concatenate([-sin, sin], 1)


def _joined(parts, out_ref):
    at = 0
    for p in parts:
        out_ref[at : at + p.shape[0], :] = p[...]
        at += p.shape[0]


def _second(*refs, strip, n, m):
    parts, (g_ref, wg_ref, wu_ref) = refs[:n], refs[n : n + 3]
    h_ref, dg_ref, du_ref, b_ref, *terms, sum_s = refs[-5 - m :]
    first, last = pl.program_id(0) == 0, pl.program_id(0) == pl.num_programs(0) - 1

    @pl.when(first)
    def _():
        _joined(parts, b_ref)
        sum_s[...] = jnp.zeros_like(sum_s)

    for at in range(0, b_ref.shape[0], strip):
        rows = slice(at, at + strip)
        gate, up = _dot(b_ref[rows, :], wg_ref[...], 1, 0), _dot(b_ref[rows, :], wu_ref[...], 1, 0)
        g = g_ref[rows, :].astype(jnp.float32)
        s = jax.nn.sigmoid(gate)
        act = gate * s
        h_ref[rows, :] = (act * up).astype(h_ref.dtype)
        du = (g * act).astype(du_ref.dtype)
        dg = (g * up * (s + act * (1 - s))).astype(dg_ref.dtype)
        du_ref[rows, :], dg_ref[rows, :] = du, dg
        sum_s[rows, :] += _dot(dg, wg_ref[...], 1, 1) + _dot(du, wu_ref[...], 1, 1)

    @pl.when(last)
    def _():
        at = 0
        for t in terms:
            t[...] = sum_s[at : at + t.shape[0], :].astype(t.dtype)
            at += t.shape[0]


def second_half(parts, d_hidden, at, wg, wu, place, whole, dtypes, held=(), bf=512, strip=512):
    rows, (d, units) = sum(p.shape[0] for p in parts), wg.shape
    out = pl.BlockSpec((rows, bf), lambda f: (place, f))
    weight = pl.BlockSpec((d, bf), lambda f: (0, f))
    once = dict(pipeline_mode=pl.Buffered(1))
    term = pl.BlockSpec((rows // len(dtypes), d), lambda f: (0, 0), **once)
    got = pl.pallas_call(
        functools.partial(_second, strip=strip, n=len(parts), m=len(dtypes)),
        grid=(units // bf,),
        in_specs=[pl.BlockSpec(p.shape, lambda f: (0, 0), **once) for p in parts]
        + [pl.BlockSpec((rows, bf), lambda f: (at, f)), weight, weight]
        + [pl.BlockSpec(memory_space=pl.ANY)] * len(held),
        out_specs=[out] * 3 + [pl.BlockSpec((rows, d), lambda f: (place, 0), **once)] + [term] * len(dtypes),
        out_shape=[jax.ShapeDtypeStruct((whole, units), wg.dtype)] * 3
        + [jax.ShapeDtypeStruct((whole, d), wg.dtype)]
        + [jax.ShapeDtypeStruct((rows // len(dtypes), d), t) for t in dtypes],
        scratch_shapes=[pltpu.VMEM((rows, d), jnp.float32)],
        input_output_aliases={len(parts) + 3 + i: i for i in range(len(held))},
        compiler_params=pltpu.CompilerParams(dimension_semantics=("arbitrary",), vmem_limit_bytes=VMEM),
        cost_estimate=pl.CostEstimate(flops=8 * rows * d * units, transcendentals=rows * units, bytes_accessed=4 * d * units + 12 * rows * units),
    )(*parts, d_hidden, wg, wu, *held)
    return got[:4], got[4:]


def _times_t(*refs, n):
    parts, w_ref, (o_ref, all_ref) = refs[:n], refs[n], refs[-2:]

    @pl.when(pl.program_id(0) == 0)
    def _():
        _joined(parts, all_ref)

    o_ref[...] = _dot(all_ref[...], w_ref[...], 1, 1).astype(o_ref.dtype)


def times_t(parts, size, w, place, whole, held=(), bf=512):
    rows, (units, d) = size * len(parts), w.shape
    block = lambda n: pl.BlockSpec((size, d), lambda f: (n, 0))
    return pl.pallas_call(
        functools.partial(_times_t, n=len(parts)),
        grid=(units // bf,),
        in_specs=[block(n) for _, n in parts]
        + [pl.BlockSpec((bf, d), lambda f: (f, 0))] + [pl.BlockSpec(memory_space=pl.ANY)] * len(held),
        out_specs=[pl.BlockSpec((rows, bf), lambda f: (0, f)), pl.BlockSpec((rows, d), lambda f: (place, 0))],
        out_shape=[jax.ShapeDtypeStruct((rows, units), w.dtype), jax.ShapeDtypeStruct((whole, d), w.dtype)],
        input_output_aliases={len(parts) + 1 + i: 1 for i in range(len(held))},
        compiler_params=pltpu.CompilerParams(dimension_semantics=("arbitrary",), vmem_limit_bytes=VMEM),
        cost_estimate=pl.CostEstimate(flops=2 * rows * d * units, transcendentals=0, bytes_accessed=2 * (d * units + rows * units + 2 * rows * d)),
    )(*(p for p, _ in parts), w, *held)


def _project(place_ref, *refs, n):
    parts, w_ref, (a_ref, o_ref) = refs[:n], refs[n], refs[-2:]

    @pl.when(pl.program_id(0) == 0)
    def _():
        at = 0
        for p in parts:
            a_ref[at : at + p.shape[0], :] = normed(p[...])
            at += p.shape[0]

    o_ref[...] = _dot(a_ref[...], w_ref[...], 1, 0).astype(o_ref.dtype)


def project(parts, w, place, whole, held=(), bf=512):
    rows, (d, columns) = sum(p.shape[0] for p in parts), w.shape
    return pl.pallas_call(
        functools.partial(_project, n=len(parts)),
        grid_spec=pltpu.PrefetchScalarGridSpec(
            num_scalar_prefetch=1,
            grid=(columns // bf,),
            in_specs=[pl.BlockSpec(p.shape, lambda f, at: (0, 0)) for p in parts]
            + [pl.BlockSpec((d, bf), lambda f, at: (0, f))] + [pl.BlockSpec(memory_space=pl.ANY)] * len(held),
            out_specs=[pl.BlockSpec((rows, d), lambda f, at: (at[0], 0)), pl.BlockSpec((rows, bf), lambda f, at: (at[0], f))],
        ),
        out_shape=[jax.ShapeDtypeStruct((whole, d), w.dtype), jax.ShapeDtypeStruct((whole, columns), w.dtype)],
        input_output_aliases={len(parts) + 2 + i: i for i in range(len(held))},
        compiler_params=pltpu.CompilerParams(dimension_semantics=("arbitrary",), vmem_limit_bytes=VMEM),
        cost_estimate=pl.CostEstimate(flops=2 * rows * d * columns, transcendentals=0, bytes_accessed=2 * (d * columns + rows * columns + 2 * rows * d)),
    )(place[None], *parts, w, *held)


def _by_rows(at_ref, h_ref, *refs):
    *parts, o_ref, turned = refs

    @pl.when(pl.program_id(0) == 0)
    def _():
        turned[...] = h_ref[...].T

    total = None
    for n, p in enumerate(parts):
        rows = pl.ds(pl.multiple_of(at_ref[n] * p.shape[0], p.shape[0]), p.shape[0])
        term = _dot(turned[:, rows], p[...], 1, 0)
        total = term if total is None else total + term
    o_ref[...] = total.astype(o_ref.dtype)


def by_rows(h, parts, at, bf=512):
    d = parts[0].shape[1]
    return pl.pallas_call(
        _by_rows,
        grid_spec=pltpu.PrefetchScalarGridSpec(
            num_scalar_prefetch=1,
            grid=(d // bf,),
            in_specs=[pl.BlockSpec(h.shape, lambda f, at: (0, 0))] + [pl.BlockSpec((p.shape[0], bf), lambda f, at: (0, f)) for p in parts],
            out_specs=pl.BlockSpec((h.shape[1], bf), lambda f, at: (0, f)),
            scratch_shapes=[pltpu.VMEM((h.shape[1], h.shape[0]), h.dtype)],
        ),
        out_shape=jax.ShapeDtypeStruct((h.shape[1], d), h.dtype),
        compiler_params=pltpu.CompilerParams(dimension_semantics=("arbitrary",), vmem_limit_bytes=VMEM),
        cost_estimate=pl.CostEstimate(flops=2 * h.size * d, transcendentals=0, bytes_accessed=2 * (h.size + h.shape[0] * d + h.shape[1] * d)),
    )(at, h, *parts)


def blank(rows, columns):
    return pl.pallas_call(lambda o: None, out_specs=pl.BlockSpec(memory_space=pl.ANY), out_shape=jax.ShapeDtypeStruct((rows, columns), jnp.bfloat16))()


def low(t):
    return t.astype(jnp.bfloat16)


def high(t):
    return t.astype(jnp.float32)


def dot(a, b):
    return _dot(a, b, 1, 0)


def dot_t(a, b):
    return _dot(a, b, 1, 1)


def dot_w(a, b):
    return low(_dot(a, b, 0, 0))


def halves(t):
    n = t.shape[0] // 2
    return [t[:n], t[n:]]


def whole(parts):
    return jnp.concatenate(parts, axis=0)


def scale_of(wide):
    return lax.rsqrt(jnp.mean(wide**2, -1, keepdims=True) + 1e-6)


def normed(h):
    wide = high(h)
    return low(wide * scale_of(wide))


def settle(terms, h, t):
    wide = high(h)
    g, scale = sum(high(x) for x in terms), scale_of(wide)
    back = low(scale * g - wide * (scale**3 * jnp.mean(g * wide, -1, keepdims=True)))
    return low(high(t) + high(back))


class Ring:
    def __init__(self, n):
        self.n = n
        self.up = [(i, (i + 1) % n) for i in range(n)]
        self.down = [(i, (i - 1) % n) for i in range(n)]

    dtypes = {0: (jnp.float32, jnp.float32), 1: (jnp.float32, jnp.bfloat16), 2: (jnp.bfloat16, jnp.bfloat16), 3: (jnp.bfloat16, jnp.float32)}

    def to_next(self, t):
        return lax.ppermute(t, "tp", self.up)

    def to_last(self, t):
        return lax.ppermute(t, "tp", self.down)

    def gather(self, parts):
        from_last = [self.to_next(p) for p in parts]
        from_next = [self.to_last(p) for p in parts]
        opposite = [self.to_next(from_last[0]), self.to_last(from_next[1])]
        return {0: parts, 1: from_next, 2: opposite, 3: from_last}

    def gather_whole(self, t):
        from_last, from_next = self.to_next(t), self.to_last(t)
        opposite = [self.to_next(halves(from_last)[0]), self.to_last(halves(from_next)[1])]
        return {0: [t], 1: [from_next], 2: opposite, 3: [from_last]}

    def exchange(self, parts):
        h = halves(parts[2])
        mid_u, mid_d = self.to_next(h[0]), self.to_last(h[1])
        from_last, from_next = self.to_next(parts[1]), self.to_last(parts[3])
        far = whole([self.to_next(mid_u), self.to_last(mid_d)])
        return {0: parts[0], 1: from_next, 2: far, 3: from_last}

    def scatter(self, term):
        from_last = {1: self.to_next(low(term(1, 1)))}
        from_next = {0: self.to_last(low(term(3, 0)))}
        a = self.to_next(low(term(2, 0)))
        b = self.to_last(low(term(2, 1)))
        from_last[0] = self.to_next(low(high(term(1, 0)) + high(a)))
        from_next[1] = self.to_last(low(high(term(3, 1)) + high(b)))
        return [(term(0, i), from_last[i], from_next[i]) for i in (0, 1)]

    def scatter_after(self, term):
        far = halves(term(2))
        a, b = self.to_next(low(far[0])), self.to_last(low(far[1]))
        one, three = halves(term(1)), halves(term(3))
        from_last = self.to_next(low(whole([one[0] + high(a), one[1]])))
        from_next = self.to_last(low(whole([three[0], three[1] + high(b)])))
        return [term(0), from_last, from_next]


ORDER = (0, 3, 1, 2)
PIECES = (((3, 0), (1, 1)), ((3, 1), (1, 0)), ((0, 0), (0, 1)), ((2, 0), (2, 1)))


def layer(ring, pairs, x, dy, w):
    tokens, _ = x.shape
    half = tokens // 2
    me = lax.axis_index("tp")
    at = lambda r: lax.rem(me + r, ring.n) * tokens
    all_tokens = ring.n * tokens

    def placed(chunks):
        out = blank(all_tokens, chunks[0].shape[1])
        for r in ORDER:
            out = lax.dynamic_update_slice(out, chunks[r], (at(r), 0))
        return out

    def of(t, r):
        return lax.dynamic_slice_in_dim(t, at(r), tokens, 0)

    shard = w["wo"].shape[0]
    part = shard // 2
    core = lax.rem(lax.axis_index("dp"), 2)
    mine = lax.dynamic_slice_in_dim(w["wo"], core * part, part, 0)
    wo_parts = ring.gather(halves(mine))
    xs = ring.gather(halves(x))
    wqkv = jnp.concatenate([w["wq"], w["wk"], w["wv"]], axis=1)
    cos, sin = angles(all_tokens)
    mine = whole([p for r in range(ring.n) for p in wo_parts[r]])
    other = lax.ppermute(mine, "dp", pairs)
    columns = lambda t, c: lax.dynamic_slice_in_dim(t, c * part, part, 1)

    held = ()
    for r in ORDER:
        held = project(xs[r], wqkv, lax.rem(me + r, ring.n), all_tokens, held)
    all_a, qkv = held
    d_y = {(r, i): (p[i], 0) if len(p) > 1 else (p[0], i) for r, p in ring.gather_whole(dy).items() for i in (0, 1)}
    heads, lse, q, k = attend(qkv, cos, sin)
    got = ring.exchange({r: of(heads, r) for r in ORDER})
    got_mine, got_other = (jnp.concatenate([columns(got[r], c) for r in range(ring.n)], axis=1) for c in (core, 1 - core))
    out = low(dot(got_mine, mine) + dot(got_other, other))
    h = low(high(x) + high(out))
    normed_h = halves(normed(h))

    d_hidden, all_d_y = {}, ()
    for ns in ((2,), (0, 1), (3,)):
        got, *all_d_y = times_t([d_y[at] for n in ns for at in PIECES[n]], half, w["w_down"], ns[0], all_tokens, all_d_y)
        d_hidden.update({n: (got, i) for i, n in enumerate(ns)})
    b = ring.gather(normed_h)
    held, d_b = (), {}
    for n in (2, 0, 1, 3):
        held, terms = second_half(
            [b[r][i] for r, i in PIECES[n]], *d_hidden[n], w["w_gate"], w["w_up"], n, all_tokens, [ring.dtypes[r][i] for r, i in PIECES[n]], held
        )
        d_b.update(zip(PIECES[n], terms))
    hidden, d_gate, d_up, all_b = held
    sums = ring.scatter(lambda r, i: d_b[r, i])
    d_h = [settle(*t) for t in zip(sums, halves(h), halves(dy))]
    by = {}
    for name, s, t in (("w_down", hidden, all_d_y[0]), ("w_gate", all_b, d_gate), ("w_up", all_b, d_up)):
        by[name] = dot_w(s, t)

    rows = whole(d_h)
    by_mine, by_other = low(dot_t(rows, mine)), low(dot_t(rows, other))

    def to_send(r):
        m, o = (t[:, r * part : (r + 1) * part] for t in (by_mine, by_other))
        return jnp.concatenate([jnp.where(core == 0, m, o), jnp.where(core == 0, o, m)], axis=1)

    d_heads = placed(ring.exchange({r: to_send(r) for r in ORDER}))
    d_hs = ring.gather(d_h)
    d_qkv = attend_back(q, k, qkv, d_heads, heads, lse, cos, sin)
    d_a = {}
    for r in (2, 3, 1, 0):
        d_a[r] = lax.optimization_barrier(dot_t(of(d_qkv, r), wqkv)) if r == 0 else dot_t(of(d_qkv, r), wqkv)
    sums = ring.scatter_after(lambda r: d_a[r])
    d_x = settle(sums, x, whole(d_h))
    blocks = jnp.stack([2 * lax.rem(me + r, ring.n) + i for r in ORDER for i in (0, 1)])
    by["wo"] = by_rows(heads, [p for r in ORDER for p in d_hs[r]], blocks)
    for i, name in enumerate(("wq", "wk", "wv")):
        by[name] = dot_w(all_a, d_qkv[:, i * shard : (i + 1) * shard])
    return d_x, by


def solution(mesh):
    ring = Ring(mesh.shape["tp"])
    pairs = [(i, i + 1 - 2 * (i % 2)) for i in range(mesh.shape["dp"])]

    def step(x, dy, *weights):
        by_x, by_w = layer(ring, pairs, x[0], dy[0], dict(zip(NAMES, weights, strict=True)))
        return (by_x[None], *(by_w[name] for name in NAMES))

    states, by_columns, by_rows = P("dp", "tp", None), P(None, "tp"), P("tp", None)
    weights = (by_columns, by_columns, by_columns, by_rows, by_columns, by_columns, by_rows)
    own = tuple(P("dp", "tp") if spec == by_columns else P(("dp", "tp"), None) for spec in weights)
    return jax.shard_map(step, mesh=mesh, in_specs=(states, states, *weights), out_specs=(states, *own), check_vma=False)
```
